32 devices in a mesh: outer: 4 (over y, x), inner: 8 (over z, core).
Axes of the slice: x: 2, y: 2, z: 4, core: 2. Of those that a mesh axis runs over, the one named last changes fastest.
Arguments:
- prim: float32 [8, 384, 512], P(None, ('outer', 'inner')), may hold values from -4 to 9, as said below
- new_owner: int32 [384], replicated, may hold values from 0 to 31, as said below
- new_slot: int32 [384], replicated, may hold values from 0 to 23, as said below
Outputs:
- placed: float32 [8, 768, 512], P(None, ('outer', 'inner'))
The draws below stay inside these ranges and needn't reach their ends.
Inputs may be any that keep to these rules, and one draw needn't show every extreme that they name: `prim`: field 0 (density) lies in 0.3 to 3 and field 4 (pressure) in 0.2 to 9; fields 1 to 3 are velocities and 5 to 7 the magnetic field. `new_owner`: block g's owner lies in the segment of 8 devices that holds device g // 12 and differs from g // 12 by at most one; owners never fall along g, so every device gets a run of consecutive blocks (possibly none); at most 6 blocks of one device go to each neighbour, and in every draw some device of each segment receives 24 blocks. `new_slot`: the blocks of one owner have slots 0, 1, 2, ... in the order of g.
All inputs are finite; a program needn't handle non-finite values.
Results may differ from the reference program's by a relative error of at most 0.0003.
Values sent between devices are 32-bit elements; how exact they have to be, the bound alone decides.
A program may use at most 64 MiB of HBM per device.

```python
import math
import jax
import jax.numpy as jnp
from jax import lax

BE = 8
GY = 16
BLK_DEV = 12
MOVE = 6
CAP = 24
CELLS = 512
NBLK = 384
SEGMENTS = 4
RANKS = 8


def assignment(key):
    base = jax.random.fold_in(key, 7)
    shift_key, pick_key = jax.random.split(base)
    offsets = jax.random.randint(shift_key, (SEGMENTS, RANKS), -MOVE, MOVE + 1)
    chosen = jax.random.randint(pick_key, (SEGMENTS, 1), 1, RANKS - 1)
    ranks_row = jnp.arange(RANKS, dtype=jnp.int32)[None, :]
    offsets = jnp.where(ranks_row == chosen, -MOVE, offsets)
    offsets = jnp.where(ranks_row == chosen + 1, MOVE, offsets)
    offsets = jnp.where(ranks_row == 0, 0, offsets)
    starts = BLK_DEV * ranks_row + offsets
    local_ids = jnp.arange(RANKS * BLK_DEV, dtype=jnp.int32)
    owner_local = jnp.sum((starts[:, None, :] <= local_ids[None, :, None]).astype(jnp.int32), axis=2) - 1
    start_of = jnp.take_along_axis(starts, owner_local, axis=1)
    slot_ids = local_ids[None, :] - start_of
    owners = owner_local + RANKS * jnp.arange(SEGMENTS, dtype=jnp.int32)[:, None]
    return (owners.reshape(-1).astype(jnp.int32), slot_ids.reshape(-1).astype(jnp.int32))


def draw_new_owner(key, part):
    return assignment(key)[0]


def draw_new_slot(key, part):
    return assignment(key)[1]


def draw_prim(key, part):
    keys = jax.random.split(jax.random.fold_in(key, 31), 4)
    shape = (NBLK, CELLS)
    position = jnp.arange(NBLK, dtype=jnp.float32)[:, None] / max(NBLK - 1, 1)
    density = jnp.exp(jax.random.uniform(keys[0], shape, jnp.float32, math.log(0.5), math.log(2.0)))
    velocity = jnp.clip(0.5 * jax.random.normal(keys[1], (3,) + shape, jnp.float32), -3.0, 3.0)
    pressure = jnp.exp(jax.random.uniform(keys[2], shape, jnp.float32, math.log(0.2), math.log(1.0))) * (1.0 + 2.0 * position)
    magnetic = jnp.clip(0.7 * jax.random.normal(keys[3], (3,) + shape, jnp.float32), -4.0, 4.0)
    return jnp.concatenate([density[None], velocity, pressure[None], magnetic], 0).astype(jnp.float32)


def setup_inputs(seed: int = 0) -> dict:
    splits = jax.random.split(jax.random.key(seed), 4)
    return {
        "prim": draw_prim(jax.random.fold_in(splits[3], 71), 0),
        "new_owner": draw_new_owner(jax.random.fold_in(splits[3], 71), 0),
        "new_slot": draw_new_slot(jax.random.fold_in(splits[3], 71), 0),
    }


GAMMA = 5.0 / 3.0
COURANT = 0.8

def minmod(former, latter):
    return 0.5 * (jnp.sign(former) + jnp.sign(latter)) * jnp.minimum(jnp.abs(former), jnp.abs(latter))

def unpack(state):
    return [state[component] for component in range(8)]

def conserved(state):
    density, speed_x, speed_y, speed_z, pressure, field_x, field_y, field_z = unpack(state)
    kinetic = 0.5 * density * (speed_x * speed_x + speed_y * speed_y + speed_z * speed_z)
    magnetic = 0.5 * (field_x * field_x + field_y * field_y + field_z * field_z)
    energy = pressure / (GAMMA - 1.0) + kinetic + magnetic
    return jnp.stack([density, density * speed_x, density * speed_y, density * speed_z, energy, field_x, field_y, field_z])

def signal(state):
    density, speed_x, speed_y, speed_z, pressure, field_x, field_y, field_z = unpack(state)
    field_sq = field_x * field_x + field_y * field_y + field_z * field_z
    return jnp.abs(speed_x) + jnp.abs(speed_y) + jnp.abs(speed_z) + 3.0 * jnp.sqrt((GAMMA * pressure + field_sq) / density)

def flux_parts(state, normal):
    density, speed_x, speed_y, speed_z, pressure, field_x, field_y, field_z = unpack(state)
    velocity = (speed_x, speed_y, speed_z)
    magnetic = (field_x, field_y, field_z)
    normal_speed = velocity[normal]
    normal_field = magnetic[normal]
    field_sq = field_x * field_x + field_y * field_y + field_z * field_z
    total_pressure = pressure + 0.5 * field_sq
    conserved_state = conserved(state)
    vel_dot_field = speed_x * field_x + speed_y * field_y + speed_z * field_z
    momentum = []
    for component in range(3):
        momentum_term = density * velocity[component] * normal_speed - magnetic[component] * normal_field
        if component == normal:
            momentum_term = momentum_term + total_pressure
        momentum.append(momentum_term)
    induction = [magnetic[component] * normal_speed - velocity[component] * normal_field for component in range(3)]
    energy_flux = (conserved_state[4] + total_pressure) * normal_speed - normal_field * vel_dot_field
    flux_terms = jnp.stack([density * normal_speed] + momentum + [energy_flux] + induction)
    signal_speed = jnp.abs(normal_speed) + jnp.sqrt((GAMMA * pressure + field_sq) / density)
    return (flux_terms, signal_speed, conserved_state)

def divergence(padded, normal):
    cell_axis = normal + 1
    inner_count = padded.shape[cell_axis] - 4

    def window(values, offset, length):
        return lax.slice_in_dim(values, offset, offset + length, axis=cell_axis)
    steps_between = window(padded, 1, inner_count + 3) - window(padded, 0, inner_count + 3)
    slopes = minmod(window(steps_between, 0, inner_count + 2), window(steps_between, 1, inner_count + 2))
    centres = window(padded, 1, inner_count + 2)
    left_state = window(centres, 0, inner_count + 1) + 0.5 * window(slopes, 0, inner_count + 1)
    right_state = window(centres, 1, inner_count + 1) - 0.5 * window(slopes, 1, inner_count + 1)
    flux_left, speed_left, state_left = flux_parts(left_state, normal)
    flux_right, speed_right, state_right = flux_parts(right_state, normal)
    face_flux = 0.5 * (flux_left + flux_right) - 0.5 * jnp.maximum(speed_left, speed_right)[None] * (state_right - state_left)
    return window(face_flux, 1, inner_count) - window(face_flux, 0, inner_count)

def advance(x_padded, y_padded, z_padded, time_step):
    middle = x_padded[:, 2:-2]
    change = divergence(x_padded, 0) + divergence(y_padded, 1) + divergence(z_padded, 2)
    return conserved(middle) - time_step * change

def pencil_of(prim, device):
    edge_len = BE
    blocks_here = lax.dynamic_slice_in_dim(prim, (device * BLK_DEV).astype(jnp.int32), BLK_DEV, 1)
    shaped = blocks_here.reshape(8, BLK_DEV, edge_len, edge_len, edge_len).transpose(0, 2, 3, 1, 4)
    return shaped.reshape(8, edge_len, edge_len, BLK_DEV * edge_len)

def reference(prim, new_owner, new_slot):
    edge_len = BE
    devices_all = prim.shape[1] // BLK_DEV
    indices = jnp.arange(devices_all, dtype=jnp.int32)
    fastest = jnp.max(lax.map(lambda device: jnp.max(signal(pencil_of(prim, device))), indices))
    time_step = COURANT / fastest

    def update(device):
        middle = pencil_of(prim, device)
        under_rows = pencil_of(prim, (device - 1) % devices_all)[:, :, edge_len - 2:]
        over_rows = pencil_of(prim, (device + 1) % devices_all)[:, :, :2]
        y_padded = jnp.concatenate([under_rows, middle, over_rows], 2)
        before_x = pencil_of(prim, (device - GY) % devices_all)[:, edge_len - 2:]
        after_x = pencil_of(prim, (device + GY) % devices_all)[:, :2]
        x_padded = jnp.concatenate([before_x, middle, after_x], 1)
        z_padded = jnp.concatenate([middle[..., -2:], middle, middle[..., :2]], 3)
        result = advance(x_padded, y_padded, z_padded, time_step)
        result = result.reshape(8, edge_len, edge_len, BLK_DEV, edge_len).transpose(0, 3, 1, 2, 4)
        return result.reshape(8, BLK_DEV, edge_len ** 3)
    updated = lax.map(update, indices)
    updated = updated.transpose(1, 0, 2, 3).reshape(8, prim.shape[1], edge_len ** 3)
    target = new_owner * CAP + new_slot
    placed = jnp.zeros((8, devices_all * CAP, edge_len ** 3), jnp.float32).at[:, target].set(updated)
    return placed
```

```python
import functools

import jax
import jax.numpy as jnp
from jax import lax
from jax.experimental import pallas as pl
from jax.experimental.pallas import tpu as pltpu
from jax.sharding import PartitionSpec as P

BE = 8
GY = 16
LANES = 128

GAMMA = 5.0 / 3.0
COURANT = 0.8
MESH = pl.DeviceIdType.MESH


def turn(value, by):
    return pltpu.roll(value, by % LANES, 1)


def half_slope(former, latter):
    low = jnp.minimum(former, latter)
    high = jnp.maximum(former, latter)
    return 0.5 * (jnp.maximum(low, 0.0) + jnp.minimum(high, 0.0))


def sound(density, pressure, field_sq):
    total = GAMMA * pressure + field_sq
    return total * lax.rsqrt(total * density)


def flux_parts(state, normal):
    density, pressure = state[0], state[4]
    vel = state[1:4]
    mag = state[5:8]
    vn, bn = vel[normal], mag[normal]
    field_sq = mag[0] * mag[0] + mag[1] * mag[1] + mag[2] * mag[2]
    speed_sq = vel[0] * vel[0] + vel[1] * vel[1] + vel[2] * vel[2]
    half_field = 0.5 * field_sq
    energy = pressure * (1.0 / (GAMMA - 1.0)) + 0.5 * density * speed_sq + half_field
    total_pressure = pressure + half_field
    vel_dot = vel[0] * mag[0] + vel[1] * mag[1] + vel[2] * mag[2]
    mom = [density * v for v in vel]
    flux_mom = []
    for k in range(3):
        term = mom[k] * vn - mag[k] * bn
        if k == normal:
            term = term + total_pressure
        flux_mom.append(term)
    induction = [None if k == normal else mag[k] * vn - vel[k] * bn for k in range(3)]
    flux = [mom[normal]] + flux_mom + [(energy + total_pressure) * vn - bn * vel_dot] + induction
    speed = jnp.abs(vn) + sound(density, pressure, field_sq)
    return flux, speed, [density] + mom + [energy] + list(mag)


def face_flux(left, right, normal):
    flux_l, speed_l, cons_l = flux_parts(left, normal)
    flux_r, speed_r, cons_r = flux_parts(right, normal)
    half = 0.5 * jnp.maximum(speed_l, speed_r)
    out = []
    for k in range(8):
        upwind = half * (cons_r[k] - cons_l[k])
        if flux_l[k] is None:
            out.append(-upwind)
        else:
            out.append(0.5 * (flux_l[k] + flux_r[k]) - upwind)
    return out


def conserved(state):
    density, pressure = state[0], state[4]
    vel, mag = state[1:4], state[5:8]
    kinetic = 0.5 * density * (vel[0] * vel[0] + vel[1] * vel[1] + vel[2] * vel[2])
    magnetic = 0.5 * (mag[0] * mag[0] + mag[1] * mag[1] + mag[2] * mag[2])
    energy = pressure * (1.0 / (GAMMA - 1.0)) + kinetic + magnetic
    return [density] + [density * v for v in vel] + [energy] + list(mag)


def step_kernel(
    count_o, count_i, blocks, reach,
    prim, own, lower, upper,
    wrap, change, x_before, x_after, y_send, y_before, y_after,
    top_send, top_in, top_send2, top_in2, move_low, move_high,
    x_sem, y_sem, in_sem, out_sem, low_sem, high_sem,
):
    tiles = prim.shape[2] // LANES
    total = count_o * count_i
    o, i = lax.axis_index("outer"), lax.axis_index("inner")
    me = o * count_i + i

    def place_of(step):
        flat = lax.rem(me + (step % total), total)
        return (lax.div(flat, count_i), lax.rem(flat, count_i))

    inner_ids = [(o, lax.rem(i + k, count_i)) for k in range(1, count_i)]
    outer_ids = [(lax.rem(o + k, count_o), i) for k in range(1, count_o)]
    greeted = inner_ids + outer_ids + [place_of(s) for s in (1, -1, GY, -GY)]
    barrier = pltpu.get_barrier_semaphore()
    for target in greeted:
        pl.semaphore_signal(barrier, inc=1, device_id=target, device_id_type=MESH)

    def send(src, dst, sems, index, target):
        copy = pltpu.make_async_remote_copy(
            src_ref=src, dst_ref=dst, send_sem=sems.at[0, index], recv_sem=sems.at[1, index],
            device_id=target, device_id_type=MESH,
        )
        return copy

    def lanes(t):
        return pl.ds(t * LANES, LANES)

    def load(t):
        return [prim[f, :, lanes(t)] for f in range(8)]

    lane = lax.broadcasted_iota(jnp.int32, (blocks, LANES), 1)
    quarter = lax.rem(lane, 64) // 16
    first_half = lane < 64
    even = lax.rem(lane, 16) < 8
    y_of = lax.rem(lane, 64) // 8
    z_of = lax.rem(lane, 8)
    y_first, y_last = y_of == 0, y_of == BE - 1
    z_first, z_last = z_of == 0, z_of == BE - 1

    top = None
    for t in range(tiles):
        w = load(t)
        field_sq = w[5] * w[5] + w[6] * w[6] + w[7] * w[7]
        signal = jnp.abs(w[1]) + jnp.abs(w[2]) + jnp.abs(w[3]) + 3.0 * sound(w[0], w[4], field_sq)
        top = signal if top is None else jnp.maximum(top, signal)
    top_send[...] = jnp.max(top, axis=0, keepdims=True)

    for f in range(8):
        low = high = None
        for t in range(tiles):
            w = prim[f, :, lanes(t)]
            a, b = turn(w, 16 * t), turn(w, 16 * t - 48)
            low = a if low is None else jnp.where(quarter == t, a, low)
            high = b if high is None else jnp.where(quarter == t, b, high)
        y_send[0, f] = low
        y_send[1, f] = high
    for f in range(8):
        wrap[f, pl.ds(1, blocks), :] = prim[f]
        wrap[f, pl.ds(0, 1), :] = prim[f, pl.ds(blocks - 1, 1), :]
        wrap[f, pl.ds(blocks + 1, 1), :] = prim[f, pl.ds(0, 1), :]

    pl.semaphore_wait(barrier, len(greeted))

    last = lanes(tiles - 1)
    x_copies = [
        send(prim.at[:, :, last], x_before, x_sem, 0, place_of(GY)),
        send(prim.at[:, :, lanes(0)], x_after, x_sem, 1, place_of(-GY)),
    ]
    y_copies = [
        send(y_send.at[1], y_before, y_sem, 0, place_of(1)),
        send(y_send.at[0], y_after, y_sem, 1, place_of(-1)),
    ]
    in_copies = [
        send(top_send, top_in.at[k], in_sem, k, inner_ids[k]) for k in range(count_i - 1)
    ]
    for copy in y_copies + in_copies + x_copies:
        copy.start()

    def next_row(v):
        return jnp.concatenate([v[1:], v[:1]], axis=0)

    def prev_row(v):
        return jnp.concatenate([v[blocks - 1 :], v[: blocks - 1]], axis=0)

    for t in range(tiles):
        w = load(t)
        left, right = [], []
        for f in range(8):
            up = jnp.where(z_last, turn(wrap[f, pl.ds(2, blocks), lanes(t)], 7), turn(w[f], -1))
            down = jnp.where(z_first, turn(wrap[f, pl.ds(0, blocks), lanes(t)], -7), turn(w[f], 1))
            h = half_slope(w[f] - down, up - w[f])
            r = w[f] - h
            left.append(w[f] + h)
            right.append(jnp.where(z_last, turn(next_row(r), 7), turn(r, -1)))
        g = face_flux(left, right, 2)
        for f in range(8):
            before = jnp.where(z_first, turn(prev_row(g[f]), -7), turn(g[f], 1))
            change[f, :, lanes(t)] = g[f] - before

    for copy in in_copies:
        copy.wait()
    row = top_send[...]
    for k in range(count_i - 1):
        row = jnp.maximum(row, top_in[k])
    top_send2[...] = row
    out_copies = [
        send(top_send2, top_in2.at[k], out_sem, k, outer_ids[k]) for k in range(count_o - 1)
    ]
    for copy in out_copies:
        copy.start()

    for copy in x_copies:
        copy.wait()

    def cells_x(t):
        if t < 0:
            return [x_before[f] for f in range(8)]
        if t >= tiles:
            return [x_after[f] for f in range(8)]
        return load(t)

    def shift_x(low_tile, high_tile):
        return turn(jnp.where(first_half, low_tile, high_tile), 64)

    here = cells_x(-1)
    dp_prev = g_prev = None
    held = None
    for t in range(-1, tiles + 1):
        after = cells_x(t + 1) if t < tiles else here
        left, right, dps = [], [], []
        for f in range(8):
            dp = shift_x(after[f], here[f]) - here[f]
            dm = shift_x(dp, dp if dp_prev is None else dp_prev[f])
            h = half_slope(dm, dp)
            dps.append(dp)
            left.append(here[f] + h)
            right.append(here[f] - h)
        if held is not None:
            old_left, old_right = held
            g = face_flux(old_left, [shift_x(right[f], old_right[f]) for f in range(8)], 0)
            if g_prev is not None:
                for f in range(8):
                    spot = (f, slice(None), lanes(t - 1))
                    change[spot] = change[spot] + (g[f] - shift_x(g[f], g_prev[f]))
            g_prev = g
        held = (left, right)
        dp_prev = dps
        here = after

    for copy in y_copies:
        copy.wait()
    ghosts = []
    left, right = [], []
    for f in range(8):
        low_own, high_own = y_send[0, f], y_send[1, f]
        before, after = y_before[f], y_after[f]
        a = jnp.where(even, high_own, turn(before, 72))
        b = jnp.where(even, turn(high_own, -8), turn(before, 64))
        c = jnp.where(even, after, turn(low_own, 72))
        d = jnp.where(even, turn(after, -8), turn(low_own, 64))
        mid = c - b
        left.append(b + half_slope(b - a, mid))
        right.append(c - half_slope(mid, d - c))
        ghosts.append(jnp.where(even, c, b))
    edge = face_flux(left, right, 1)

    for copy in out_copies:
        copy.wait()
    row = top_send2[...]
    for k in range(count_o - 1):
        row = jnp.maximum(row, top_in2[k])
    time_step = COURANT / jnp.max(row, axis=1, keepdims=True)

    to_low = [
        send(move_low.at[:, :, lanes(t)], upper.at[:, :, lanes(t)], low_sem, t, (o, lax.rem(i + count_i - 1, count_i)))
        for t in range(tiles)
    ]
    to_high = [
        send(move_high.at[:, :, lanes(t)], lower.at[:, :, lanes(t)], high_sem, t, (o, lax.rem(i + 1, count_i)))
        for t in range(tiles)
    ]
    for t in range(tiles):
        w = load(t)
        back = 56 - 16 * t
        left, right = [], []
        for f in range(8):
            ghost = turn(ghosts[f], back)
            up = jnp.where(y_last, ghost, turn(w[f], -8))
            down = jnp.where(y_first, ghost, turn(w[f], 8))
            h = half_slope(w[f] - down, up - w[f])
            left.append(w[f] + h)
            right.append(turn(w[f] - h, -8))
        g = face_flux(left, right, 1)
        cons = conserved(w)
        for f in range(8):
            rim = turn(edge[f], back)
            face = jnp.where(y_last, rim, g[f])
            before = jnp.where(y_first, rim, turn(g[f], 8))
            result = cons[f] - time_step * (change[f, :, lanes(t)] + (face - before))
            own[f, :, lanes(t)] = result
            move_low[f, :, lanes(t)] = result[:reach]
            move_high[f, :, lanes(t)] = result[blocks - reach :]

        @pl.when(i > 0)
        def _():
            to_low[t].start()

        @pl.when(i < count_i - 1)
        def _():
            to_high[t].start()

    @pl.when(i > 0)
    def _():
        for t in range(tiles):
            to_low[t].wait_send()
            to_high[t].wait_recv()

    @pl.when(i < count_i - 1)
    def _():
        for t in range(tiles):
            to_high[t].wait_send()
            to_low[t].wait_recv()


def place_kernel(blocks, reach, block_total, count_i, owner, own, lower, upper, out, wide):
    me = lax.axis_index("outer") * count_i + lax.axis_index("inner")
    capacity = blocks + 2 * reach
    start = jnp.int32(capacity)
    count = jnp.int32(0)
    for c in range(capacity):
        g = me * blocks - reach + c
        inside = (g >= 0) & (g < block_total)
        mine = inside & (owner[jnp.clip(g, 0, block_total - 1)] == me)
        count = count + mine.astype(jnp.int32)
        start = jnp.where(mine, jnp.minimum(start, c), start)
    start = jnp.where(count > 0, start, 0)
    row = lax.broadcasted_iota(jnp.int32, (capacity, own.shape[2]), 0)
    live = row < count
    for f in range(8):
        wide[f, pl.ds(0, reach), :] = lower[f]
        wide[f, pl.ds(reach, blocks), :] = own[f]
        wide[f, pl.ds(reach + blocks, reach), :] = upper[f]
    for f in range(8):
        out[f] = jnp.where(live, pltpu.roll(wide[f], capacity - start, 0), 0.0)


def per_device(count_o, count_i, prim, new_owner, new_slot):
    blocks, cells = prim.shape[1:]
    reach = blocks // 2
    tiles = cells // LANES
    vmem = pl.BlockSpec(memory_space=pltpu.VMEM)
    f32 = jnp.float32
    dma = pltpu.SemaphoreType.DMA
    own, lower, upper = pl.pallas_call(
        functools.partial(step_kernel, count_o, count_i, blocks, reach),
        out_shape=[
            jax.ShapeDtypeStruct((8, blocks, cells), f32),
            jax.ShapeDtypeStruct((8, reach, cells), f32),
            jax.ShapeDtypeStruct((8, reach, cells), f32),
        ],
        in_specs=[vmem],
        out_specs=[vmem] * 3,
        scratch_shapes=[
            pltpu.VMEM((8, blocks + 4, cells), f32),
            pltpu.VMEM((8, blocks, cells), f32),
            pltpu.VMEM((8, blocks, LANES), f32),
            pltpu.VMEM((8, blocks, LANES), f32),
            pltpu.VMEM((2, 8, blocks, LANES), f32),
            pltpu.VMEM((8, blocks, LANES), f32),
            pltpu.VMEM((8, blocks, LANES), f32),
            pltpu.VMEM((1, LANES), f32),
            pltpu.VMEM((count_i - 1, 1, LANES), f32),
            pltpu.VMEM((1, LANES), f32),
            pltpu.VMEM((count_o - 1, 1, LANES), f32),
            pltpu.VMEM((8, reach, cells), f32),
            pltpu.VMEM((8, reach, cells), f32),
            dma((2, 2)),
            dma((2, 2)),
            dma((2, count_i - 1)),
            dma((2, count_o - 1)),
            dma((2, tiles)),
            dma((2, tiles)),
        ],
        compiler_params=pltpu.CompilerParams(collective_id=0, has_side_effects=True),
        name="step",
    )(prim)
    capacity = blocks + 2 * reach
    return pl.pallas_call(
        functools.partial(place_kernel, blocks, reach, new_owner.shape[0], count_i),
        out_shape=jax.ShapeDtypeStruct((8, capacity, cells), f32),
        in_specs=[pl.BlockSpec(memory_space=pltpu.SMEM), vmem, vmem, vmem],
        out_specs=vmem,
        scratch_shapes=[pltpu.VMEM((8, capacity, cells), f32)],
        name="place",
    )(new_owner, own, lower, upper)


def solution(mesh):
    in_specs = (P(None, ("outer", "inner"), None), P(), P())
    out_specs = P(None, ("outer", "inner"), None)
    run = functools.partial(per_device, mesh.shape["outer"], mesh.shape["inner"])
    return jax.shard_map(
        run, mesh=mesh, in_specs=in_specs, out_specs=out_specs, check_vma=False
    )
```

```python
import functools

import jax
import jax.numpy as jnp
from jax import lax
from jax.experimental import pallas as pl
from jax.experimental.pallas import tpu as pltpu
from jax.sharding import PartitionSpec as P

BE = 8
GY = 16
LANES = 128

GAMMA = 5.0 / 3.0
COURANT = 0.8
MESH = pl.DeviceIdType.MESH


def turn(value, by):
    return pltpu.roll(value, by % LANES if isinstance(by, int) else by, 1)


def half_slope(former, latter):
    low = jnp.minimum(former, latter)
    high = jnp.maximum(former, latter)
    return 0.5 * (jnp.maximum(low, 0.0) + jnp.minimum(high, 0.0))


def sound(density, pressure, field_sq):
    total = GAMMA * pressure + field_sq
    return total * lax.rsqrt(total * density)


def flux_parts(state, normal):
    density, pressure = state[0], state[4]
    vel = state[1:4]
    mag = state[5:8]
    vn, bn = vel[normal], mag[normal]
    field_sq = mag[0] * mag[0] + mag[1] * mag[1] + mag[2] * mag[2]
    speed_sq = vel[0] * vel[0] + vel[1] * vel[1] + vel[2] * vel[2]
    half_field = 0.5 * field_sq
    energy = pressure * (1.0 / (GAMMA - 1.0)) + 0.5 * density * speed_sq + half_field
    total_pressure = pressure + half_field
    vel_dot = vel[0] * mag[0] + vel[1] * mag[1] + vel[2] * mag[2]
    mom = [density * v for v in vel]
    flux_mom = []
    for k in range(3):
        term = mom[k] * vn - mag[k] * bn
        if k == normal:
            term = term + total_pressure
        flux_mom.append(term)
    induction = [None if k == normal else mag[k] * vn - vel[k] * bn for k in range(3)]
    flux = [mom[normal]] + flux_mom + [(energy + total_pressure) * vn - bn * vel_dot] + induction
    speed = jnp.abs(vn) + sound(density, pressure, field_sq)
    return flux, speed, [density] + mom + [energy] + list(mag)


def face_flux(left, right, normal):
    flux_l, speed_l, cons_l = flux_parts(left, normal)
    flux_r, speed_r, cons_r = flux_parts(right, normal)
    half = 0.5 * jnp.maximum(speed_l, speed_r)
    out = []
    for k in range(8):
        upwind = half * (cons_r[k] - cons_l[k])
        if flux_l[k] is None:
            out.append(-upwind)
        else:
            out.append(0.5 * (flux_l[k] + flux_r[k]) - upwind)
    return out


def conserved(state):
    density, pressure = state[0], state[4]
    vel, mag = state[1:4], state[5:8]
    kinetic = 0.5 * density * (vel[0] * vel[0] + vel[1] * vel[1] + vel[2] * vel[2])
    magnetic = 0.5 * (mag[0] * mag[0] + mag[1] * mag[1] + mag[2] * mag[2])
    energy = pressure * (1.0 / (GAMMA - 1.0)) + kinetic + magnetic
    return [density] + [density * v for v in vel] + [energy] + list(mag)


def step_kernel(
    count_o, count_i, blocks, reach,
    prim, moved,
    raw, tile, change, left, right, faces, x_before, x_after, y_send, y_before, y_after, ghost, edge,
    top_send, top_in, top_send2, top_in2,
    load_sem, x_sem, y_sem, in_sem, out_sem, low_sem, high_sem,
):
    tiles = raw.shape[0]
    total = count_o * count_i
    o, i = lax.axis_index("outer"), lax.axis_index("inner")
    me = o * count_i + i
    loads = [
        pltpu.make_async_copy(prim.at[:, pl.ds(t * LANES, LANES)], raw.at[t], load_sem.at[t])
        for t in range(tiles)
    ]
    for copy in loads:
        copy.start()

    def place_of(step):
        flat = lax.rem(me + (step % total), total)
        return (lax.div(flat, count_i), lax.rem(flat, count_i))

    def inner_id(k):
        return (o, lax.rem(i + 1 + k, count_i))

    def outer_id(k):
        return (lax.rem(o + 1 + k, count_o), i)

    barrier = pltpu.get_barrier_semaphore()

    def greet(target):
        pl.semaphore_signal(barrier, inc=1, device_id=target, device_id_type=MESH)

    @pl.loop(0, count_i - 1)
    def _(k):
        greet(inner_id(k))

    @pl.loop(0, count_o - 1)
    def _(k):
        greet(outer_id(k))

    for s in (1, -1, GY, -GY):
        greet(place_of(s))
    greeted = count_i + count_o + 2

    def send(src, dst, sems, index, target):
        return pltpu.make_async_remote_copy(
            src_ref=src, dst_ref=dst, send_sem=sems.at[0, index], recv_sem=sems.at[1, index],
            device_id=target, device_id_type=MESH,
        )

    lane = lax.broadcasted_iota(jnp.int32, (blocks, LANES), 1)
    quarter = lax.rem(lane, 64) // 16
    first_half = lane < 64
    even = lax.rem(lane, 16) < 8
    y_of = lax.rem(lane, 64) // 8
    z_of = lax.rem(lane, 8)
    y_first, y_last = y_of == 0, y_of == BE - 1
    z_first, z_last = z_of == 0, z_of == BE - 1

    for copy in loads:
        copy.wait()

    def gather(t, top):
        w = [raw[t, pl.ds(f, blocks, 8), :] for f in range(8)]
        for f in range(8):
            tile[t + 1, f] = w[f]
            a, b = turn(w[f], 16 * t), turn(w[f], lax.rem(16 * t + 80, LANES))
            mine = quarter == t
            y_send[0, f] = jnp.where(mine, a, y_send[0, f])
            y_send[1, f] = jnp.where(mine, b, y_send[1, f])
        field_sq = w[5] * w[5] + w[6] * w[6] + w[7] * w[7]
        signal = jnp.abs(w[1]) + jnp.abs(w[2]) + jnp.abs(w[3]) + 3.0 * sound(w[0], w[4], field_sq)
        return jnp.maximum(top, signal)

    top = lax.fori_loop(0, tiles, gather, jnp.zeros((blocks, LANES), jnp.float32))
    top_send[...] = jnp.max(top, axis=0, keepdims=True)
    pl.semaphore_wait(barrier, greeted)

    x_copies = [
        send(raw.at[tiles - 1], x_before, x_sem, 0, place_of(GY)),
        send(raw.at[0], x_after, x_sem, 1, place_of(-GY)),
    ]
    y_copies = [
        send(y_send.at[1], y_before, y_sem, 0, place_of(1)),
        send(y_send.at[0], y_after, y_sem, 1, place_of(-1)),
    ]
    for copy in y_copies:
        copy.start()

    def in_copy(k):
        return send(top_send, top_in.at[k], in_sem, k, inner_id(k))

    def out_copy(k):
        return send(top_send2, top_in2.at[k], out_sem, k, outer_id(k))

    @pl.loop(0, count_i - 1)
    def _(k):
        in_copy(k).start()

    for copy in x_copies:
        copy.start()

    def next_row(v):
        return jnp.concatenate([v[1:], v[:1]], axis=0)

    def prev_row(v):
        return jnp.concatenate([v[blocks - 1 :], v[: blocks - 1]], axis=0)

    @pl.loop(0, tiles)
    def _(t):
        lefts, rights = [], []
        for f in range(8):
            w = tile[t + 1, f]
            up = jnp.where(z_last, turn(next_row(w), 7), turn(w, -1))
            down = jnp.where(z_first, turn(prev_row(w), -7), turn(w, 1))
            h = half_slope(w - down, up - w)
            r = w - h
            lefts.append(w + h)
            rights.append(jnp.where(z_last, turn(next_row(r), 7), turn(r, -1)))
        g = face_flux(lefts, rights, 2)
        for f in range(8):
            before = jnp.where(z_first, turn(prev_row(g[f]), -7), turn(g[f], 1))
            change[t, f] = g[f] - before

    @pl.loop(0, count_i - 1)
    def _(k):
        in_copy(k).wait()

    row = top_send[...]
    for k in range(count_i - 1):
        row = jnp.maximum(row, top_in[k])
    top_send2[...] = row

    @pl.loop(0, count_o - 1)
    def _(k):
        out_copy(k).start()

    for copy in x_copies:
        copy.wait()
    for f in range(8):
        tile[0, f] = x_before[pl.ds(f, blocks, 8), :]
        tile[tiles + 1, f] = x_after[pl.ds(f, blocks, 8), :]

    def shift_x(low_tile, high_tile):
        return turn(jnp.where(first_half, low_tile, high_tile), 64)

    @pl.loop(0, tiles + 2)
    def _(t):
        over, under = jnp.minimum(t + 1, tiles + 1), jnp.maximum(t - 1, 0)
        for f in range(8):
            w = tile[t, f]
            up = shift_x(tile[over, f], w)
            down = shift_x(w, tile[under, f])
            h = half_slope(w - down, up - w)
            left[t, f] = w + h
            right[t, f] = w - h

    @pl.loop(0, tiles + 1)
    def _(t):
        g = face_flux(
            [left[t, f] for f in range(8)],
            [shift_x(right[t + 1, f], right[t, f]) for f in range(8)],
            0,
        )
        for f in range(8):
            faces[t, f] = g[f]

    for copy in y_copies:
        copy.wait()
    lefts, rights = [], []
    for f in range(8):
        low_own, high_own = y_send[0, f], y_send[1, f]
        before, after = y_before[f], y_after[f]
        a = jnp.where(even, high_own, turn(before, 72))
        b = jnp.where(even, turn(high_own, -8), turn(before, 64))
        c = jnp.where(even, after, turn(low_own, 72))
        d = jnp.where(even, turn(after, -8), turn(low_own, 64))
        mid = c - b
        lefts.append(b + half_slope(b - a, mid))
        rights.append(c - half_slope(mid, d - c))
        ghost[f] = jnp.where(even, c, b)
    g = face_flux(lefts, rights, 1)
    for f in range(8):
        edge[f] = g[f]

    @pl.loop(0, count_o - 1)
    def _(k):
        out_copy(k).wait()

    row = top_send2[...]
    for k in range(count_o - 1):
        row = jnp.maximum(row, top_in2[k])
    time_step = COURANT / jnp.max(row, axis=1, keepdims=True)

    low_rows = pl.ds(reach * 8, reach * 8)
    high_rows = pl.ds(blocks * 8, reach * 8)
    to_low_rows = pl.ds((reach + blocks) * 8, reach * 8)
    to_high_rows = pl.ds(0, reach * 8)

    def to_low(t):
        target = (o, lax.rem(i + count_i - 1, count_i))
        return send(moved.at[t, low_rows], moved.at[t, to_low_rows], low_sem, t, target)

    def to_high(t):
        target = (o, lax.rem(i + 1, count_i))
        return send(moved.at[t, high_rows], moved.at[t, to_high_rows], high_sem, t, target)

    @pl.loop(0, tiles)
    def _(t):
        back = lax.rem(56 + LANES - 16 * t, LANES)
        lefts, rights, w = [], [], []
        for f in range(8):
            w.append(tile[t + 1, f])
            rim = turn(ghost[f], back)
            up = jnp.where(y_last, rim, turn(w[f], -8))
            down = jnp.where(y_first, rim, turn(w[f], 8))
            h = half_slope(w[f] - down, up - w[f])
            lefts.append(w[f] + h)
            rights.append(turn(w[f] - h, -8))
        g = face_flux(lefts, rights, 1)
        cons = conserved(w)
        for f in range(8):
            rim = turn(edge[f], back)
            face = jnp.where(y_last, rim, g[f])
            before = jnp.where(y_first, rim, turn(g[f], 8))
            across = faces[t + 1, f]
            across = across - shift_x(across, faces[t, f])
            result = cons[f] - time_step * (across + (face - before) + change[t, f])
            moved[t, pl.ds(reach * 8 + f, blocks, 8), :] = result

        @pl.when(i > 0)
        def _():
            to_low(t).start()

        @pl.when(i < count_i - 1)
        def _():
            to_high(t).start()

    @pl.when(i > 0)
    def _():
        for t in range(tiles):
            to_low(t).wait_send()
            to_high(t).wait_recv()

    @pl.when(i < count_i - 1)
    def _():
        for t in range(tiles):
            to_high(t).wait_send()
            to_low(t).wait_recv()


def place_kernel(blocks, reach, block_total, count_i, owner, moved, out, wide, held, in_sem, out_sem):
    me = lax.axis_index("outer") * count_i + lax.axis_index("inner")
    capacity = blocks + 2 * reach
    fetch = pltpu.make_async_copy(moved, wide.at[:, pl.ds(0, capacity * 8)], in_sem)
    fetch.start()

    def look(c, carry):
        start, count = carry
        g = me * blocks - reach + c
        inside = (g >= 0) & (g < block_total)
        mine = inside & (owner[jnp.clip(g, 0, block_total - 1)] == me)
        return jnp.where(mine, jnp.minimum(start, c), start), count + mine.astype(jnp.int32)

    start, count = lax.fori_loop(0, capacity, look, (jnp.int32(2 * reach), jnp.int32(0)))
    live = lax.broadcasted_iota(jnp.int32, (capacity, LANES), 0) < count
    fetch.wait()

    def put(f):
        return pltpu.make_async_copy(held.at[f], out.at[f], out_sem.at[f])

    @pl.loop(0, 8)
    def _(f):
        for t in range(wide.shape[0]):
            held[f, :, t * LANES : (t + 1) * LANES] = jnp.where(
                live, wide[t, pl.ds(start * 8 + f, capacity, 8), :], 0.0
            )
        put(f).start()

    @pl.loop(0, 8)
    def _(f):
        put(f).wait()


def per_device(count_o, count_i, prim, new_owner, new_slot):
    blocks, cells = prim.shape[1:]
    reach = blocks // 2
    tiles = cells // LANES
    capacity = blocks + 2 * reach
    anywhere = pl.BlockSpec(memory_space=pl.ANY)
    vmem = pl.BlockSpec(memory_space=pltpu.VMEM)
    f32 = jnp.float32
    dma = pltpu.SemaphoreType.DMA

    def room(*lead):
        return pltpu.VMEM(lead + (8, blocks, LANES), f32)

    rows = prim.transpose(1, 0, 2).reshape(blocks * 8, cells)
    moved = pl.pallas_call(
        functools.partial(step_kernel, count_o, count_i, blocks, reach),
        out_shape=jax.ShapeDtypeStruct((tiles, capacity * 8, LANES), f32),
        in_specs=[anywhere],
        out_specs=vmem,
        scratch_shapes=[
            pltpu.VMEM((tiles, blocks * 8, LANES), f32),
            room(tiles + 2),
            room(tiles),
            room(tiles + 2),
            room(tiles + 2),
            room(tiles + 1),
            pltpu.VMEM((blocks * 8, LANES), f32),
            pltpu.VMEM((blocks * 8, LANES), f32),
            room(2),
            room(),
            room(),
            room(),
            room(),
            pltpu.VMEM((1, LANES), f32),
            pltpu.VMEM((count_i - 1, 1, LANES), f32),
            pltpu.VMEM((1, LANES), f32),
            pltpu.VMEM((count_o - 1, 1, LANES), f32),
            dma((tiles,)),
            dma((2, 2)),
            dma((2, 2)),
            dma((2, count_i - 1)),
            dma((2, count_o - 1)),
            dma((2, tiles)),
            dma((2, tiles)),
        ],
        compiler_params=pltpu.CompilerParams(collective_id=0, has_side_effects=True),
        name="step",
    )(rows)
    return pl.pallas_call(
        functools.partial(place_kernel, blocks, reach, new_owner.shape[0], count_i),
        out_shape=jax.ShapeDtypeStruct((8, capacity, cells), f32),
        in_specs=[pl.BlockSpec(memory_space=pltpu.SMEM), anywhere],
        out_specs=anywhere,
        scratch_shapes=[
            pltpu.VMEM((tiles, (capacity + 2 * reach) * 8, LANES), f32),
            pltpu.VMEM((8, capacity, cells), f32),
            dma,
            dma((8,)),
        ],
        name="place",
    )(new_owner, moved)


def solution(mesh):
    in_specs = (P(None, ("outer", "inner"), None), P(), P())
    out_specs = P(None, ("outer", "inner"), None)
    run = functools.partial(per_device, mesh.shape["outer"], mesh.shape["inner"])
    return jax.shard_map(
        run, mesh=mesh, in_specs=in_specs, out_specs=out_specs, check_vma=False
    )
```

```python
import functools

import jax
import jax.numpy as jnp
from jax import lax
from jax.experimental import pallas as pl
from jax.experimental.pallas import tpu as pltpu
from jax.sharding import PartitionSpec as P

BE = 8
GY = 16
LANES = 128

GAMMA = 5.0 / 3.0
COURANT = 0.8
MESH = pl.DeviceIdType.MESH


def turn(value, by):
    return pltpu.roll(value, by % LANES if isinstance(by, int) else by, 1)


def half_slope(former, latter):
    low = jnp.minimum(former, latter)
    high = jnp.maximum(former, latter)
    return 0.5 * (jnp.maximum(low, 0.0) + jnp.minimum(high, 0.0))


def sound(density, pressure, field_sq):
    total = GAMMA * pressure + field_sq
    return total * lax.rsqrt(total * density)


def flux_parts(state, normal):
    density, pressure = state[0], state[4]
    vel = state[1:4]
    mag = state[5:8]
    vn, bn = vel[normal], mag[normal]
    field_sq = mag[0] * mag[0] + mag[1] * mag[1] + mag[2] * mag[2]
    speed_sq = vel[0] * vel[0] + vel[1] * vel[1] + vel[2] * vel[2]
    half_field = 0.5 * field_sq
    energy = pressure * (1.0 / (GAMMA - 1.0)) + 0.5 * density * speed_sq + half_field
    total_pressure = pressure + half_field
    vel_dot = vel[0] * mag[0] + vel[1] * mag[1] + vel[2] * mag[2]
    mom = [density * v for v in vel]
    flux_mom = []
    for k in range(3):
        term = mom[k] * vn - mag[k] * bn
        if k == normal:
            term = term + total_pressure
        flux_mom.append(term)
    induction = [None if k == normal else mag[k] * vn - vel[k] * bn for k in range(3)]
    flux = [mom[normal]] + flux_mom + [(energy + total_pressure) * vn - bn * vel_dot] + induction
    speed = jnp.abs(vn) + sound(density, pressure, field_sq)
    return flux, speed, [density] + mom + [energy] + list(mag)


def face_flux(left, right, normal):
    flux_l, speed_l, cons_l = flux_parts(left, normal)
    flux_r, speed_r, cons_r = flux_parts(right, normal)
    half = 0.5 * jnp.maximum(speed_l, speed_r)
    out = []
    for k in range(8):
        upwind = half * (cons_r[k] - cons_l[k])
        if flux_l[k] is None:
            out.append(-upwind)
        else:
            out.append(0.5 * (flux_l[k] + flux_r[k]) - upwind)
    return out


def conserved(state):
    density, pressure = state[0], state[4]
    vel, mag = state[1:4], state[5:8]
    kinetic = 0.5 * density * (vel[0] * vel[0] + vel[1] * vel[1] + vel[2] * vel[2])
    magnetic = 0.5 * (mag[0] * mag[0] + mag[1] * mag[1] + mag[2] * mag[2])
    energy = pressure * (1.0 / (GAMMA - 1.0)) + kinetic + magnetic
    return [density] + [density * v for v in vel] + [energy] + list(mag)


def step_kernel(
    count_o, count_i, blocks, reach,
    block_total, prim, owners, moved, state, fastest, run,
    tile, change, left, right, faces, x_before, x_after, y_send, y_before, y_after, ghost, edge,
    top_send, top_in, top_send2, top_in2,
    owner, load_sem, owner_sem, x_sem, y_sem, in_sem, out_sem, low_sem, high_sem, state_sem,
):
    tiles = state.shape[0]
    capacity = blocks + 2 * reach
    own_rows = pl.ds(reach * 8, blocks * 8)
    total = count_o * count_i
    o, i = lax.axis_index("outer"), lax.axis_index("inner")
    me = o * count_i + i
    loads = [
        pltpu.make_async_copy(prim.at[:, pl.ds(t * LANES, LANES)], state.at[t, own_rows], load_sem.at[t])
        for t in range(tiles)
    ]
    for copy in loads:
        copy.start()
    owner_load = pltpu.make_async_copy(owners, owner, owner_sem)
    owner_load.start()

    def place_of(step):
        flat = lax.rem(me + (step % total), total)
        return (lax.div(flat, count_i), lax.rem(flat, count_i))

    def inner_id(k):
        return (o, lax.rem(i + 1 + k, count_i))

    def outer_id(k):
        return (lax.rem(o + 1 + k, count_o), i)

    barrier = pltpu.get_barrier_semaphore()

    def greet(target):
        pl.semaphore_signal(barrier, inc=1, device_id=target, device_id_type=MESH)

    @pl.loop(0, count_i - 1)
    def _(k):
        greet(inner_id(k))

    @pl.loop(0, count_o - 1)
    def _(k):
        greet(outer_id(k))

    for s in (1, -1, GY, -GY):
        greet(place_of(s))
    greeted = count_i + count_o + 2

    def send(src, dst, sems, index, target):
        return pltpu.make_async_remote_copy(
            src_ref=src, dst_ref=dst, send_sem=sems.at[0, index], recv_sem=sems.at[1, index],
            device_id=target, device_id_type=MESH,
        )

    lane = lax.broadcasted_iota(jnp.int32, (blocks, LANES), 1)
    quarter = lax.rem(lane, 64) // 16
    first_half = lane < 64
    even = lax.rem(lane, 16) < 8
    y_of = lax.rem(lane, 64) // 8
    z_of = lax.rem(lane, 8)
    y_first, y_last = y_of == 0, y_of == BE - 1
    z_first, z_last = z_of == 0, z_of == BE - 1

    for copy in loads:
        copy.wait()

    def gather(t, top):
        w = [state[t, pl.ds(reach * 8 + f, blocks, 8), :] for f in range(8)]
        for f in range(8):
            tile[t + 1, f] = w[f]
            a, b = turn(w[f], 16 * t), turn(w[f], lax.rem(16 * t + 80, LANES))
            mine = quarter == t
            y_send[0, f] = jnp.where(mine, a, y_send[0, f])
            y_send[1, f] = jnp.where(mine, b, y_send[1, f])
        field_sq = w[5] * w[5] + w[6] * w[6] + w[7] * w[7]
        signal = jnp.abs(w[1]) + jnp.abs(w[2]) + jnp.abs(w[3]) + 3.0 * sound(w[0], w[4], field_sq)
        return jnp.maximum(top, signal)

    top = lax.fori_loop(0, tiles, gather, jnp.zeros((blocks, LANES), jnp.float32))
    top_send[...] = jnp.max(top, axis=0, keepdims=True)

    def next_row(v):
        return jnp.concatenate([v[1:], v[:1]], axis=0)

    def prev_row(v):
        return jnp.concatenate([v[blocks - 1 :], v[: blocks - 1]], axis=0)

    @pl.loop(0, tiles)
    def _(t):
        lefts, rights = [], []
        for f in range(8):
            w = tile[t + 1, f]
            up = jnp.where(z_last, turn(next_row(w), 7), turn(w, -1))
            down = jnp.where(z_first, turn(prev_row(w), -7), turn(w, 1))
            h = half_slope(w - down, up - w)
            r = w - h
            lefts.append(w + h)
            rights.append(jnp.where(z_last, turn(next_row(r), 7), turn(r, -1)))
        g = face_flux(lefts, rights, 2)
        for f in range(8):
            before = jnp.where(z_first, turn(prev_row(g[f]), -7), turn(g[f], 1))
            change[t, f] = g[f] - before

    pl.semaphore_wait(barrier, greeted)

    x_copies = [
        send(state.at[tiles - 1, own_rows], x_before, x_sem, 0, place_of(GY)),
        send(state.at[0, own_rows], x_after, x_sem, 1, place_of(-GY)),
    ]
    y_copies = [
        send(y_send.at[1], y_before, y_sem, 0, place_of(1)),
        send(y_send.at[0], y_after, y_sem, 1, place_of(-1)),
    ]
    for copy in y_copies:
        copy.start()

    def in_copy(k):
        return send(top_send, top_in.at[k], in_sem, k, inner_id(k))

    def out_copy(k):
        return send(top_send2, top_in2.at[k], out_sem, k, outer_id(k))

    @pl.loop(0, count_i - 1)
    def _(k):
        in_copy(k).start()

    for copy in x_copies:
        copy.start()

    low_rows = pl.ds(reach * 8, reach * 8)
    high_rows = pl.ds(blocks * 8, reach * 8)
    to_low_rows = pl.ds((reach + blocks) * 8, reach * 8)
    to_high_rows = pl.ds(0, reach * 8)

    def to_low(t):
        target = (o, lax.rem(i + count_i - 1, count_i))
        return send(moved.at[t, low_rows], moved.at[t, to_low_rows], low_sem, t, target)

    def to_high(t):
        target = (o, lax.rem(i + 1, count_i))
        return send(moved.at[t, high_rows], moved.at[t, to_high_rows], high_sem, t, target)

    state_low = send(
        state.at[:, low_rows], state.at[:, to_low_rows], state_sem, 0, (o, lax.rem(i + count_i - 1, count_i))
    )
    state_high = send(
        state.at[:, high_rows], state.at[:, to_high_rows], state_sem, 1, (o, lax.rem(i + 1, count_i))
    )

    @pl.when(i > 0)
    def _():
        state_low.start()

    @pl.when(i < count_i - 1)
    def _():
        state_high.start()

    owner_load.wait()

    def look(c, carry):
        start, count = carry
        g = me * blocks - reach + c
        inside = (g >= 0) & (g < block_total)
        mine = inside & (owner[jnp.clip(g, 0, block_total - 1)] == me)
        return jnp.where(mine, jnp.minimum(start, c), start), count + mine.astype(jnp.int32)

    start, count = lax.fori_loop(0, capacity, look, (jnp.int32(2 * reach), jnp.int32(0)))
    row_of = lax.broadcasted_iota(jnp.int32, run.shape, 0)
    run[...] = jnp.where(row_of == 0, start, count)

    @pl.loop(0, count_i - 1)
    def _(k):
        in_copy(k).wait()

    row = top_send[...]
    for k in range(count_i - 1):
        row = jnp.maximum(row, top_in[k])
    top_send2[...] = row

    @pl.loop(0, count_o - 1)
    def _(k):
        out_copy(k).start()

    for copy in x_copies:
        copy.wait()
    for f in range(8):
        tile[0, f] = x_before[pl.ds(f, blocks, 8), :]
        tile[tiles + 1, f] = x_after[pl.ds(f, blocks, 8), :]

    def shift_x(low_tile, high_tile):
        return turn(jnp.where(first_half, low_tile, high_tile), 64)

    @pl.loop(0, tiles + 2)
    def _(t):
        over, under = jnp.minimum(t + 1, tiles + 1), jnp.maximum(t - 1, 0)
        for f in range(8):
            w = tile[t, f]
            up = shift_x(tile[over, f], w)
            down = shift_x(w, tile[under, f])
            h = half_slope(w - down, up - w)
            left[t, f] = w + h
            right[t, f] = w - h

    @pl.loop(0, tiles + 1)
    def _(t):
        g = face_flux(
            [left[t, f] for f in range(8)],
            [shift_x(right[t + 1, f], right[t, f]) for f in range(8)],
            0,
        )
        for f in range(8):
            faces[t, f] = g[f]

    for copy in y_copies:
        copy.wait()
    lefts, rights = [], []
    for f in range(8):
        low_own, high_own = y_send[0, f], y_send[1, f]
        before, after = y_before[f], y_after[f]
        a = jnp.where(even, high_own, turn(before, 72))
        b = jnp.where(even, turn(high_own, -8), turn(before, 64))
        c = jnp.where(even, after, turn(low_own, 72))
        d = jnp.where(even, turn(after, -8), turn(low_own, 64))
        mid = c - b
        lefts.append(b + half_slope(b - a, mid))
        rights.append(c - half_slope(mid, d - c))
        ghost[f] = jnp.where(even, c, b)
    g = face_flux(lefts, rights, 1)
    for f in range(8):
        edge[f] = g[f]

    @pl.loop(0, tiles)
    def _(t):
        back = lax.rem(56 + LANES - 16 * t, LANES)
        lefts, rights, w = [], [], []
        for f in range(8):
            w.append(tile[t + 1, f])
            rim = turn(ghost[f], back)
            up = jnp.where(y_last, rim, turn(w[f], -8))
            down = jnp.where(y_first, rim, turn(w[f], 8))
            h = half_slope(w[f] - down, up - w[f])
            lefts.append(w[f] + h)
            rights.append(turn(w[f] - h, -8))
        g = face_flux(lefts, rights, 1)
        for f in range(8):
            rim = turn(edge[f], back)
            face = jnp.where(y_last, rim, g[f])
            before = jnp.where(y_first, rim, turn(g[f], 8))
            across = faces[t + 1, f]
            across = across - shift_x(across, faces[t, f])
            result = across + (face - before) + change[t, f]
            moved[t, pl.ds(reach * 8 + f, blocks, 8), :] = result

        @pl.when(i > 0)
        def _():
            to_low(t).start()

        @pl.when(i < count_i - 1)
        def _():
            to_high(t).start()

    @pl.loop(0, count_o - 1)
    def _(k):
        out_copy(k).wait()

    row = top_send2[...]
    for k in range(count_o - 1):
        row = jnp.maximum(row, top_in2[k])
    fastest[...] = row

    @pl.when(i > 0)
    def _():
        for t in range(tiles):
            to_low(t).wait_send()
            to_high(t).wait_recv()
        state_low.wait_send()
        state_high.wait_recv()

    @pl.when(i < count_i - 1)
    def _():
        for t in range(tiles):
            to_high(t).wait_send()
            to_low(t).wait_recv()
        state_high.wait_send()
        state_low.wait_recv()


def place_kernel(capacity, moved, state, fastest, run, out, held, out_sem):
    tiles = state.shape[0]
    start = jnp.max(run[pl.ds(0, 1), :])
    count = jnp.max(run[pl.ds(1, 1), :])
    live = lax.broadcasted_iota(jnp.int32, (capacity, LANES), 0) < count
    time_step = COURANT / jnp.max(fastest[...], axis=1, keepdims=True)

    def put(t):
        spot = pl.ds(pl.multiple_of(t * LANES, LANES), LANES)
        return pltpu.make_async_copy(held.at[t], out.at[:, :, spot], out_sem.at[t])

    @pl.loop(0, tiles)
    def _(t):
        rows = [pl.ds(start * 8 + f, capacity, 8) for f in range(8)]
        cons = conserved([state[t, rows[f], :] for f in range(8)])
        for f in range(8):
            held[t, f] = jnp.where(live, cons[f] - time_step * moved[t, rows[f], :], 0.0)
        put(t).start()

    @pl.loop(0, tiles)
    def _(t):
        put(t).wait()


def per_device(count_o, count_i, prim, new_owner, new_slot):
    blocks, cells = prim.shape[1:]
    reach = blocks // 2
    tiles = cells // LANES
    capacity = blocks + 2 * reach
    anywhere = pl.BlockSpec(memory_space=pl.ANY)
    vmem = pl.BlockSpec(memory_space=pltpu.VMEM)
    f32 = jnp.float32
    dma = pltpu.SemaphoreType.DMA

    def room(*lead):
        return pltpu.VMEM(lead + (8, blocks, LANES), f32)

    rows = prim.transpose(1, 0, 2).reshape(blocks * 8, cells)
    handed = pl.pallas_call(
        functools.partial(step_kernel, count_o, count_i, blocks, reach, new_owner.shape[0]),
        out_shape=[
            pltpu.VMEM((tiles, (capacity + 2 * reach) * 8, LANES), f32),
            pltpu.VMEM((tiles, (capacity + 2 * reach) * 8, LANES), f32),
            pltpu.VMEM((1, LANES), f32),
            pltpu.VMEM((2, LANES), jnp.int32),
        ],
        in_specs=[anywhere, anywhere],
        out_specs=[vmem] * 4,
        scratch_shapes=[
            room(tiles + 2),
            room(tiles),
            room(tiles + 2),
            room(tiles + 2),
            room(tiles + 1),
            pltpu.VMEM((blocks * 8, LANES), f32),
            pltpu.VMEM((blocks * 8, LANES), f32),
            room(2),
            room(),
            room(),
            room(),
            room(),
            pltpu.VMEM((1, LANES), f32),
            pltpu.VMEM((count_i - 1, 1, LANES), f32),
            pltpu.VMEM((1, LANES), f32),
            pltpu.VMEM((count_o - 1, 1, LANES), f32),
            pltpu.SMEM(new_owner.shape, jnp.int32),
            dma((tiles,)),
            dma,
            dma((2, 2)),
            dma((2, 2)),
            dma((2, count_i - 1)),
            dma((2, count_o - 1)),
            dma((2, tiles)),
            dma((2, tiles)),
            dma((2, 2)),
        ],
        compiler_params=pltpu.CompilerParams(collective_id=0, has_side_effects=True),
        name="step",
    )(rows, new_owner)
    return pl.pallas_call(
        functools.partial(place_kernel, capacity),
        out_shape=jax.ShapeDtypeStruct((8, capacity, cells), f32),
        in_specs=[vmem] * 4,
        out_specs=anywhere,
        scratch_shapes=[pltpu.VMEM((tiles, 8, capacity, LANES), f32), dma((tiles,))],
        name="place",
    )(*[pltpu.with_memory_space_constraint(part, pltpu.VMEM) for part in handed])


def solution(mesh):
    in_specs = (P(None, ("outer", "inner"), None), P(), P())
    out_specs = P(None, ("outer", "inner"), None)
    run = functools.partial(per_device, mesh.shape["outer"], mesh.shape["inner"])
    return jax.shard_map(
        run, mesh=mesh, in_specs=in_specs, out_specs=out_specs, check_vma=False
    )
```

```python
import functools

import jax
import jax.numpy as jnp
from jax import lax
from jax.experimental import pallas as pl
from jax.experimental.pallas import tpu as pltpu
from jax.sharding import PartitionSpec as P

BE = 8
GY = 16
LANES = 128

GAMMA = 5.0 / 3.0
COURANT = 0.8
MESH = pl.DeviceIdType.MESH


def turn(value, by):
    return pltpu.roll(value, by % LANES if isinstance(by, int) else by, 1)


def half_slope(former, latter):
    low = jnp.minimum(former, latter)
    high = jnp.maximum(former, latter)
    return 0.5 * (jnp.maximum(low, 0.0) + jnp.minimum(high, 0.0))


def sound(density, pressure, field_sq):
    total = GAMMA * pressure + field_sq
    return total * lax.rsqrt(total * density)


def flux_parts(state, normal):
    density, pressure = state[0], state[4]
    vel = state[1:4]
    mag = state[5:8]
    vn, bn = vel[normal], mag[normal]
    field_sq = mag[0] * mag[0] + mag[1] * mag[1] + mag[2] * mag[2]
    speed_sq = vel[0] * vel[0] + vel[1] * vel[1] + vel[2] * vel[2]
    half_field = 0.5 * field_sq
    energy = pressure * (1.0 / (GAMMA - 1.0)) + 0.5 * density * speed_sq + half_field
    total_pressure = pressure + half_field
    vel_dot = vel[0] * mag[0] + vel[1] * mag[1] + vel[2] * mag[2]
    mom = [density * v for v in vel]
    flux_mom = []
    for k in range(3):
        term = mom[k] * vn - mag[k] * bn
        if k == normal:
            term = term + total_pressure
        flux_mom.append(term)
    induction = [None if k == normal else mag[k] * vn - vel[k] * bn for k in range(3)]
    flux = [mom[normal]] + flux_mom + [(energy + total_pressure) * vn - bn * vel_dot] + induction
    speed = jnp.abs(vn) + sound(density, pressure, field_sq)
    return flux, speed, [density] + mom + [energy] + list(mag)


def face_flux(left, right, normal):
    flux_l, speed_l, cons_l = flux_parts(left, normal)
    flux_r, speed_r, cons_r = flux_parts(right, normal)
    half = 0.5 * jnp.maximum(speed_l, speed_r)
    out = []
    for k in range(8):
        upwind = half * (cons_r[k] - cons_l[k])
        if flux_l[k] is None:
            out.append(-upwind)
        else:
            out.append(0.5 * (flux_l[k] + flux_r[k]) - upwind)
    return out


def conserved(state):
    density, pressure = state[0], state[4]
    vel, mag = state[1:4], state[5:8]
    kinetic = 0.5 * density * (vel[0] * vel[0] + vel[1] * vel[1] + vel[2] * vel[2])
    magnetic = 0.5 * (mag[0] * mag[0] + mag[1] * mag[1] + mag[2] * mag[2])
    energy = pressure * (1.0 / (GAMMA - 1.0)) + kinetic + magnetic
    return [density] + [density * v for v in vel] + [energy] + list(mag)


def step_kernel(
    count_o, count_i, blocks, reach,
    block_total, prim, owners, moved, state, fastest, run,
    tile, change, left, right, faces, x_before, x_after, y_send, y_before, y_after, inner, edge, near,
    top_send, top_in, top_send2, top_in2,
    owner, load_sem, owner_sem, x_sem, y_sem, in_sem, out_sem, low_sem, high_sem, state_sem,
):
    tiles = state.shape[0]
    capacity = blocks + 2 * reach
    own_rows = pl.ds(reach * 8, blocks * 8)
    total = count_o * count_i
    o, i = lax.axis_index("outer"), lax.axis_index("inner")
    me = o * count_i + i
    loads = [
        pltpu.make_async_copy(prim.at[:, pl.ds(t * LANES, LANES)], state.at[t, own_rows], load_sem.at[t])
        for t in range(tiles)
    ]
    for copy in loads:
        copy.start()
    owner_load = pltpu.make_async_copy(owners, owner, owner_sem)
    owner_load.start()

    def place_of(step):
        flat = lax.rem(me + (step % total), total)
        return (lax.div(flat, count_i), lax.rem(flat, count_i))

    def inner_id(k):
        return (o, lax.rem(i + 1 + k, count_i))

    def outer_id(k):
        return (lax.rem(o + 1 + k, count_o), i)

    barrier = pltpu.get_barrier_semaphore()

    def greet(target):
        pl.semaphore_signal(barrier, inc=1, device_id=target, device_id_type=MESH)

    @pl.loop(0, count_i - 1)
    def _(k):
        greet(inner_id(k))

    @pl.loop(0, count_o - 1)
    def _(k):
        greet(outer_id(k))

    for s in (1, -1, GY, -GY):
        greet(place_of(s))
    greeted = count_i + count_o + 2

    def send(src, dst, sems, index, target):
        return pltpu.make_async_remote_copy(
            src_ref=src, dst_ref=dst, send_sem=sems.at[0, index], recv_sem=sems.at[1, index],
            device_id=target, device_id_type=MESH,
        )

    lane = lax.broadcasted_iota(jnp.int32, (blocks, LANES), 1)
    quarter = lax.rem(lane, 64) // 16
    first_half = lane < 64
    even = lax.rem(lane, 16) < 8
    y_of = lax.rem(lane, 64) // 8
    z_of = lax.rem(lane, 8)
    y_inside = (y_of >= 1) & (y_of <= BE - 3)
    y_rim = (y_of == 0) | (y_of == BE - 1)
    y_near = (y_of == 1) | (y_of == BE - 2)
    packed_tile = jnp.where(even, quarter, lax.rem(lane + 40, 64) // 16)
    z_first, z_last = z_of == 0, z_of == BE - 1

    for copy in loads:
        copy.wait()

    def gather(t, top):
        w = [state[t, pl.ds(reach * 8 + f, blocks, 8), :] for f in range(8)]
        for f in range(8):
            tile[t + 1, f] = w[f]
            a, b = turn(w[f], 16 * t), turn(w[f], lax.rem(16 * t + 80, LANES))
            mine = quarter == t
            y_send[0, f] = jnp.where(mine, a, y_send[0, f])
            y_send[1, f] = jnp.where(mine, b, y_send[1, f])
        field_sq = w[5] * w[5] + w[6] * w[6] + w[7] * w[7]
        signal = jnp.abs(w[1]) + jnp.abs(w[2]) + jnp.abs(w[3]) + 3.0 * sound(w[0], w[4], field_sq)
        return jnp.maximum(top, signal)

    top = lax.fori_loop(0, tiles, gather, jnp.zeros((blocks, LANES), jnp.float32))
    top_send[...] = jnp.max(top, axis=0, keepdims=True)

    def next_row(v):
        return jnp.concatenate([v[1:], v[:1]], axis=0)

    def prev_row(v):
        return jnp.concatenate([v[blocks - 1 :], v[: blocks - 1]], axis=0)

    @pl.loop(0, tiles)
    def _(t):
        lefts, rights = [], []
        for f in range(8):
            w = tile[t + 1, f]
            up = jnp.where(z_last, turn(next_row(w), 7), turn(w, -1))
            down = jnp.where(z_first, turn(prev_row(w), -7), turn(w, 1))
            h = half_slope(w - down, up - w)
            r = w - h
            lefts.append(w + h)
            rights.append(jnp.where(z_last, turn(next_row(r), 7), turn(r, -1)))
        g = face_flux(lefts, rights, 2)
        for f in range(8):
            before = jnp.where(z_first, turn(prev_row(g[f]), -7), turn(g[f], 1))
            change[t, f] = g[f] - before

    @pl.loop(0, tiles)
    def _(t):
        ahead = lax.rem(80 + 16 * t, LANES)
        lefts, rights = [], []
        for f in range(8):
            w = tile[t + 1, f]
            h = half_slope(w - turn(w, 8), turn(w, -8) - w)
            lefts.append(w + h)
            rights.append(turn(w - h, -8))
            beside = turn(jnp.where(y_of == 1, w - h, w + h), ahead)
            inner[f] = jnp.where(packed_tile == t, beside, inner[f])
        g = face_flux(lefts, rights, 1)
        for f in range(8):
            kept = jnp.where(y_inside, g[f], 0.0)
            change[t, f] = change[t, f] + (kept - turn(kept, 8))

    pl.semaphore_wait(barrier, greeted)

    x_copies = [
        send(state.at[tiles - 1, own_rows], x_before, x_sem, 0, place_of(GY)),
        send(state.at[0, own_rows], x_after, x_sem, 1, place_of(-GY)),
    ]
    y_copies = [
        send(y_send.at[1], y_before, y_sem, 0, place_of(1)),
        send(y_send.at[0], y_after, y_sem, 1, place_of(-1)),
    ]
    for copy in y_copies:
        copy.start()

    def in_copy(k):
        return send(top_send, top_in.at[k], in_sem, k, inner_id(k))

    def out_copy(k):
        return send(top_send2, top_in2.at[k], out_sem, k, outer_id(k))

    @pl.loop(0, count_i - 1)
    def _(k):
        in_copy(k).start()

    for copy in x_copies:
        copy.start()

    low_rows = pl.ds(reach * 8, reach * 8)
    high_rows = pl.ds(blocks * 8, reach * 8)
    to_low_rows = pl.ds((reach + blocks) * 8, reach * 8)
    to_high_rows = pl.ds(0, reach * 8)

    def to_low(t):
        target = (o, lax.rem(i + count_i - 1, count_i))
        return send(moved.at[t, low_rows], moved.at[t, to_low_rows], low_sem, t, target)

    def to_high(t):
        target = (o, lax.rem(i + 1, count_i))
        return send(moved.at[t, high_rows], moved.at[t, to_high_rows], high_sem, t, target)

    state_low = send(
        state.at[:, low_rows], state.at[:, to_low_rows], state_sem, 0, (o, lax.rem(i + count_i - 1, count_i))
    )
    state_high = send(
        state.at[:, high_rows], state.at[:, to_high_rows], state_sem, 1, (o, lax.rem(i + 1, count_i))
    )

    @pl.when(i > 0)
    def _():
        state_low.start()

    @pl.when(i < count_i - 1)
    def _():
        state_high.start()

    owner_load.wait()

    def look(c, carry):
        start, count = carry
        g = me * blocks - reach + c
        inside = (g >= 0) & (g < block_total)
        mine = inside & (owner[jnp.clip(g, 0, block_total - 1)] == me)
        return jnp.where(mine, jnp.minimum(start, c), start), count + mine.astype(jnp.int32)

    start, count = lax.fori_loop(0, capacity, look, (jnp.int32(2 * reach), jnp.int32(0)))
    row_of = lax.broadcasted_iota(jnp.int32, run.shape, 0)
    run[...] = jnp.where(row_of == 0, start, count)

    @pl.loop(0, count_i - 1)
    def _(k):
        in_copy(k).wait()

    row = top_send[...]
    for k in range(count_i - 1):
        row = jnp.maximum(row, top_in[k])
    top_send2[...] = row

    @pl.loop(0, count_o - 1)
    def _(k):
        out_copy(k).start()

    def shift_x(low_tile, high_tile):
        return turn(jnp.where(first_half, low_tile, high_tile), 64)

    @pl.loop(0, tiles + 2)
    def _(k):
        @pl.when(k == tiles - 2)
        def _():
            x_copies[0].wait()
            for f in range(8):
                tile[0, f] = x_before[pl.ds(f, blocks, 8), :]

        @pl.when(k == tiles)
        def _():
            x_copies[1].wait()
            for f in range(8):
                tile[tiles + 1, f] = x_after[pl.ds(f, blocks, 8), :]

        t = jnp.where(k < tiles, tiles - 1 - k, k)
        face = jnp.where(k < tiles, t, t - 1)
        over, under = jnp.minimum(t + 1, tiles + 1), jnp.maximum(t - 1, 0)
        for f in range(8):
            w = tile[t, f]
            up = shift_x(tile[over, f], w)
            down = shift_x(w, tile[under, f])
            h = half_slope(w - down, up - w)
            left[t, f] = w + h
            right[t, f] = w - h
        g = face_flux(
            [left[face, f] for f in range(8)],
            [shift_x(right[face + 1, f], right[face, f]) for f in range(8)],
            0,
        )
        for f in range(8):
            faces[face, f] = g[f]

    for copy in y_copies:
        copy.wait()
    lefts, rights, inner_lefts, inner_rights = [], [], [], []
    for f in range(8):
        low_own, high_own = y_send[0, f], y_send[1, f]
        before, after = y_before[f], y_after[f]
        a = jnp.where(even, high_own, turn(before, 72))
        b = jnp.where(even, turn(high_own, -8), turn(before, 64))
        c = jnp.where(even, after, turn(low_own, 72))
        d = jnp.where(even, turn(after, -8), turn(low_own, 64))
        mid = c - b
        h_b, h_c = half_slope(b - a, mid), half_slope(mid, d - c)
        lefts.append(b + h_b)
        rights.append(c - h_c)
        p = inner[f]
        p = jnp.where(even, p, turn(p, -16))
        inner_lefts.append(jnp.where(even, p, c + h_c))
        inner_rights.append(jnp.where(even, b - h_b, p))
    g = face_flux(lefts, rights, 1)
    g_inner = face_flux(inner_lefts, inner_rights, 1)
    for f in range(8):
        between = g[f] - g_inner[f]
        edge[f] = jnp.where(even, between, -between)
        near[f] = jnp.where(even, g_inner[f], -turn(g_inner[f], 16))

    @pl.loop(0, tiles)
    def _(t):
        rim_back = lax.rem(56 + LANES - 16 * t, LANES)
        near_back = lax.rem(48 + LANES - 16 * t, LANES)
        for f in range(8):
            across = faces[t + 1, f]
            across = across - shift_x(across, faces[t, f])
            added = jnp.where(
                y_rim, turn(edge[f], rim_back), jnp.where(y_near, turn(near[f], near_back), 0.0)
            )
            result = across + (change[t, f] + added)
            moved[t, pl.ds(reach * 8 + f, blocks, 8), :] = result

        @pl.when(i > 0)
        def _():
            to_low(t).start()

        @pl.when(i < count_i - 1)
        def _():
            to_high(t).start()

    @pl.loop(0, count_o - 1)
    def _(k):
        out_copy(k).wait()

    row = top_send2[...]
    for k in range(count_o - 1):
        row = jnp.maximum(row, top_in2[k])
    fastest[...] = row

    @pl.when(i > 0)
    def _():
        for t in range(tiles):
            to_low(t).wait_send()
            to_high(t).wait_recv()
        state_low.wait_send()
        state_high.wait_recv()

    @pl.when(i < count_i - 1)
    def _():
        for t in range(tiles):
            to_high(t).wait_send()
            to_low(t).wait_recv()
        state_high.wait_send()
        state_low.wait_recv()


def place_kernel(capacity, moved, state, fastest, run, out, held, out_sem):
    tiles = state.shape[0]
    start = jnp.max(run[pl.ds(0, 1), :])
    count = jnp.max(run[pl.ds(1, 1), :])
    live = lax.broadcasted_iota(jnp.int32, (capacity, LANES), 0) < count
    time_step = COURANT / jnp.max(fastest[...], axis=1, keepdims=True)

    def put(t):
        spot = pl.ds(pl.multiple_of(t * LANES, LANES), LANES)
        return pltpu.make_async_copy(held.at[t], out.at[:, :, spot], out_sem.at[t])

    @pl.loop(0, tiles)
    def _(t):
        rows = [pl.ds(start * 8 + f, capacity, 8) for f in range(8)]
        cons = conserved([state[t, rows[f], :] for f in range(8)])
        for f in range(8):
            held[t, f] = jnp.where(live, cons[f] - time_step * moved[t, rows[f], :], 0.0)
        put(t).start()

    @pl.loop(0, tiles)
    def _(t):
        put(t).wait()


def per_device(count_o, count_i, prim, new_owner, new_slot):
    blocks, cells = prim.shape[1:]
    reach = blocks // 2
    tiles = cells // LANES
    capacity = blocks + 2 * reach
    anywhere = pl.BlockSpec(memory_space=pl.ANY)
    vmem = pl.BlockSpec(memory_space=pltpu.VMEM)
    f32 = jnp.float32
    dma = pltpu.SemaphoreType.DMA

    def room(*lead):
        return pltpu.VMEM(lead + (8, blocks, LANES), f32)

    rows = prim.transpose(1, 0, 2).reshape(blocks * 8, cells)
    handed = pl.pallas_call(
        functools.partial(step_kernel, count_o, count_i, blocks, reach, new_owner.shape[0]),
        out_shape=[
            pltpu.VMEM((tiles, (capacity + 2 * reach) * 8, LANES), f32),
            pltpu.VMEM((tiles, (capacity + 2 * reach) * 8, LANES), f32),
            pltpu.VMEM((1, LANES), f32),
            pltpu.VMEM((2, LANES), jnp.int32),
        ],
        in_specs=[anywhere, anywhere],
        out_specs=[vmem] * 4,
        scratch_shapes=[
            room(tiles + 2),
            room(tiles),
            room(tiles + 2),
            room(tiles + 2),
            room(tiles + 1),
            pltpu.VMEM((blocks * 8, LANES), f32),
            pltpu.VMEM((blocks * 8, LANES), f32),
            room(2),
            room(),
            room(),
            room(),
            room(),
            room(),
            pltpu.VMEM((1, LANES), f32),
            pltpu.VMEM((count_i - 1, 1, LANES), f32),
            pltpu.VMEM((1, LANES), f32),
            pltpu.VMEM((count_o - 1, 1, LANES), f32),
            pltpu.SMEM(new_owner.shape, jnp.int32),
            dma((tiles,)),
            dma,
            dma((2, 2)),
            dma((2, 2)),
            dma((2, count_i - 1)),
            dma((2, count_o - 1)),
            dma((2, tiles)),
            dma((2, tiles)),
            dma((2, 2)),
        ],
        compiler_params=pltpu.CompilerParams(collective_id=0, has_side_effects=True),
        name="step",
    )(rows, new_owner)
    return pl.pallas_call(
        functools.partial(place_kernel, capacity),
        out_shape=jax.ShapeDtypeStruct((8, capacity, cells), f32),
        in_specs=[vmem] * 4,
        out_specs=anywhere,
        scratch_shapes=[pltpu.VMEM((tiles, 8, capacity, LANES), f32), dma((tiles,))],
        name="place",
    )(*[pltpu.with_memory_space_constraint(part, pltpu.VMEM) for part in handed])


def solution(mesh):
    in_specs = (P(None, ("outer", "inner"), None), P(), P())
    out_specs = P(None, ("outer", "inner"), None)
    run = functools.partial(per_device, mesh.shape["outer"], mesh.shape["inner"])
    return jax.shard_map(
        run, mesh=mesh, in_specs=in_specs, out_specs=out_specs, check_vma=False
    )
```

```python
import functools

import jax
import jax.numpy as jnp
from jax import lax
from jax.experimental import pallas as pl
from jax.experimental.pallas import tpu as pltpu
from jax.sharding import PartitionSpec as P

BE = 8
GY = 16
LANES = 128

GAMMA = 5.0 / 3.0
COURANT = 0.8
MESH = pl.DeviceIdType.MESH


def turn(value, by):
    return pltpu.roll(value, by % LANES if isinstance(by, int) else by, 1)


def half_slope(former, latter):
    low = jnp.minimum(former, latter)
    high = jnp.maximum(former, latter)
    return 0.5 * (jnp.maximum(low, 0.0) + jnp.minimum(high, 0.0))


def sound(density, pressure, field_sq):
    total = GAMMA * pressure + field_sq
    return total * lax.rsqrt(total * density)


def flux_parts(state, normal):
    density, pressure = state[0], state[4]
    vel = state[1:4]
    mag = state[5:8]
    vn, bn = vel[normal], mag[normal]
    field_sq = mag[0] * mag[0] + mag[1] * mag[1] + mag[2] * mag[2]
    speed_sq = vel[0] * vel[0] + vel[1] * vel[1] + vel[2] * vel[2]
    half_field = 0.5 * field_sq
    energy = pressure * (1.0 / (GAMMA - 1.0)) + 0.5 * density * speed_sq + half_field
    total_pressure = pressure + half_field
    vel_dot = vel[0] * mag[0] + vel[1] * mag[1] + vel[2] * mag[2]
    mom = [density * v for v in vel]
    flux_mom = []
    for k in range(3):
        term = mom[k] * vn - mag[k] * bn
        if k == normal:
            term = term + total_pressure
        flux_mom.append(term)
    induction = [None if k == normal else mag[k] * vn - vel[k] * bn for k in range(3)]
    flux = [mom[normal]] + flux_mom + [(energy + total_pressure) * vn - bn * vel_dot] + induction
    speed = jnp.abs(vn) + sound(density, pressure, field_sq)
    return flux, speed, [density] + mom + [energy] + list(mag)


def face_flux(left, right, normal):
    flux_l, speed_l, cons_l = flux_parts(left, normal)
    flux_r, speed_r, cons_r = flux_parts(right, normal)
    half = 0.5 * jnp.maximum(speed_l, speed_r)
    out = []
    for k in range(8):
        upwind = half * (cons_r[k] - cons_l[k])
        if flux_l[k] is None:
            out.append(-upwind)
        else:
            out.append(0.5 * (flux_l[k] + flux_r[k]) - upwind)
    return out


def conserved(state):
    density, pressure = state[0], state[4]
    vel, mag = state[1:4], state[5:8]
    kinetic = 0.5 * density * (vel[0] * vel[0] + vel[1] * vel[1] + vel[2] * vel[2])
    magnetic = 0.5 * (mag[0] * mag[0] + mag[1] * mag[1] + mag[2] * mag[2])
    energy = pressure * (1.0 / (GAMMA - 1.0)) + kinetic + magnetic
    return [density] + [density * v for v in vel] + [energy] + list(mag)


def step_kernel(
    count_o, count_i, blocks, reach,
    block_total, prim, owners, moved, state, fastest, run,
    tile, change, left, right, faces, x_before, x_after, y_send, y_before, y_after, inner, edge, near,
    top_send, top_in, top_send2, top_in2,
    owner, load_sem, owner_sem, x_sem, y_sem, in_sem, out_sem, low_sem, high_sem, state_sem,
):
    tiles = state.shape[0]
    capacity = blocks + 2 * reach
    own_rows = pl.ds(reach * 8, blocks * 8)
    total = count_o * count_i
    o, i = lax.axis_index("outer"), lax.axis_index("inner")
    me = o * count_i + i
    loads = [
        pltpu.make_async_copy(prim.at[:, pl.ds(t * LANES, LANES)], state.at[t, own_rows], load_sem.at[t])
        for t in range(tiles)
    ]
    for copy in loads:
        copy.start()
    owner_load = pltpu.make_async_copy(owners, owner, owner_sem)
    owner_load.start()

    def place_of(step):
        flat = lax.rem(me + (step % total), total)
        return (lax.div(flat, count_i), lax.rem(flat, count_i))

    def inner_id(k):
        return (o, lax.rem(i + 1 + k, count_i))

    def outer_id(k):
        return (lax.rem(o + 1 + k, count_o), i)

    barrier = pltpu.get_barrier_semaphore()

    def greet(target):
        pl.semaphore_signal(barrier, inc=1, device_id=target, device_id_type=MESH)

    @pl.loop(0, count_i - 1)
    def _(k):
        greet(inner_id(k))

    @pl.loop(0, count_o - 1)
    def _(k):
        greet(outer_id(k))

    for s in (1, -1, GY, -GY):
        greet(place_of(s))
    greeted = count_i + count_o + 2

    def send(src, dst, sems, index, target):
        return pltpu.make_async_remote_copy(
            src_ref=src, dst_ref=dst, send_sem=sems.at[0, index], recv_sem=sems.at[1, index],
            device_id=target, device_id_type=MESH,
        )

    lane = lax.broadcasted_iota(jnp.int32, (blocks, LANES), 1)
    quarter = lax.rem(lane, 64) // 16
    first_half = lane < 64
    even = lax.rem(lane, 16) < 8
    y_of = lax.rem(lane, 64) // 8
    z_of = lax.rem(lane, 8)
    y_inside = (y_of >= 1) & (y_of <= BE - 3)
    y_rim = (y_of == 0) | (y_of == BE - 1)
    y_near = (y_of == 1) | (y_of == BE - 2)
    packed_tile = jnp.where(even, quarter, lax.rem(lane + 40, 64) // 16)
    z_first, z_last = z_of == 0, z_of == BE - 1

    for copy in loads:
        copy.wait()

    def gather(t, top):
        w = [state[t, pl.ds(reach * 8 + f, blocks, 8), :] for f in range(8)]
        for f in range(8):
            tile[t + 1, f] = w[f]
            a, b = turn(w[f], 16 * t), turn(w[f], lax.rem(16 * t + 80, LANES))
            mine = quarter == t
            y_send[0, f] = jnp.where(mine, a, y_send[0, f])
            y_send[1, f] = jnp.where(mine, b, y_send[1, f])
        field_sq = w[5] * w[5] + w[6] * w[6] + w[7] * w[7]
        signal = jnp.abs(w[1]) + jnp.abs(w[2]) + jnp.abs(w[3]) + 3.0 * sound(w[0], w[4], field_sq)
        return jnp.maximum(top, signal)

    top = lax.fori_loop(0, tiles, gather, jnp.zeros((blocks, LANES), jnp.float32))
    top_send[...] = jnp.max(top, axis=0, keepdims=True)

    pl.semaphore_wait(barrier, greeted)

    x_copies = [
        send(state.at[tiles - 1, own_rows], x_before, x_sem, 0, place_of(GY)),
        send(state.at[0, own_rows], x_after, x_sem, 1, place_of(-GY)),
    ]
    y_copies = [
        send(y_send.at[1], y_before, y_sem, 0, place_of(1)),
        send(y_send.at[0], y_after, y_sem, 1, place_of(-1)),
    ]
    for copy in y_copies:
        copy.start()

    def in_copy(k):
        return send(top_send, top_in.at[k], in_sem, k, inner_id(k))

    def out_copy(k):
        return send(top_send2, top_in2.at[k], out_sem, k, outer_id(k))

    @pl.loop(0, count_i - 1)
    def _(k):
        in_copy(k).start()

    for copy in x_copies:
        copy.start()

    low_rows = pl.ds(reach * 8, reach * 8)
    high_rows = pl.ds(blocks * 8, reach * 8)
    to_low_rows = pl.ds((reach + blocks) * 8, reach * 8)
    to_high_rows = pl.ds(0, reach * 8)

    def to_low(t):
        target = (o, lax.rem(i + count_i - 1, count_i))
        return send(moved.at[t, low_rows], moved.at[t, to_low_rows], low_sem, t, target)

    def to_high(t):
        target = (o, lax.rem(i + 1, count_i))
        return send(moved.at[t, high_rows], moved.at[t, to_high_rows], high_sem, t, target)

    state_low = send(
        state.at[:, low_rows], state.at[:, to_low_rows], state_sem, 0, (o, lax.rem(i + count_i - 1, count_i))
    )
    state_high = send(
        state.at[:, high_rows], state.at[:, to_high_rows], state_sem, 1, (o, lax.rem(i + 1, count_i))
    )

    @pl.when(i > 0)
    def _():
        state_low.start()

    @pl.when(i < count_i - 1)
    def _():
        state_high.start()

    owner_load.wait()

    def look(c, carry):
        start, count = carry
        g = me * blocks - reach + c
        inside = (g >= 0) & (g < block_total)
        mine = inside & (owner[jnp.clip(g, 0, block_total - 1)] == me)
        return jnp.where(mine, jnp.minimum(start, c), start), count + mine.astype(jnp.int32)

    start, count = lax.fori_loop(0, capacity, look, (jnp.int32(2 * reach), jnp.int32(0)))
    row_of = lax.broadcasted_iota(jnp.int32, run.shape, 0)
    run[...] = jnp.where(row_of == 0, start, count)

    def next_row(v):
        return jnp.concatenate([v[1:], v[:1]], axis=0)

    def prev_row(v):
        return jnp.concatenate([v[blocks - 1 :], v[: blocks - 1]], axis=0)

    @pl.loop(0, tiles)
    def _(t):
        lefts, rights = [], []
        for f in range(8):
            w = tile[t + 1, f]
            up = jnp.where(z_last, turn(next_row(w), 7), turn(w, -1))
            down = jnp.where(z_first, turn(prev_row(w), -7), turn(w, 1))
            h = half_slope(w - down, up - w)
            r = w - h
            lefts.append(w + h)
            rights.append(jnp.where(z_last, turn(next_row(r), 7), turn(r, -1)))
        g = face_flux(lefts, rights, 2)
        for f in range(8):
            before = jnp.where(z_first, turn(prev_row(g[f]), -7), turn(g[f], 1))
            change[t, f] = g[f] - before

    @pl.loop(0, tiles)
    def _(t):
        ahead = lax.rem(80 + 16 * t, LANES)
        lefts, rights = [], []
        for f in range(8):
            w = tile[t + 1, f]
            h = half_slope(w - turn(w, 8), turn(w, -8) - w)
            lefts.append(w + h)
            rights.append(turn(w - h, -8))
            beside = turn(jnp.where(y_of == 1, w - h, w + h), ahead)
            inner[f] = jnp.where(packed_tile == t, beside, inner[f])
        g = face_flux(lefts, rights, 1)
        for f in range(8):
            kept = jnp.where(y_inside, g[f], 0.0)
            change[t, f] = change[t, f] + (kept - turn(kept, 8))

    @pl.loop(0, count_i - 1)
    def _(k):
        in_copy(k).wait()

    row = top_send[...]
    for k in range(count_i - 1):
        row = jnp.maximum(row, top_in[k])
    top_send2[...] = row

    @pl.loop(0, count_o - 1)
    def _(k):
        out_copy(k).start()

    def shift_x(low_tile, high_tile):
        return turn(jnp.where(first_half, low_tile, high_tile), 64)

    @pl.loop(0, tiles + 2)
    def _(k):
        @pl.when(k == tiles - 2)
        def _():
            x_copies[0].wait()
            for f in range(8):
                tile[0, f] = x_before[pl.ds(f, blocks, 8), :]

        @pl.when(k == tiles)
        def _():
            x_copies[1].wait()
            for f in range(8):
                tile[tiles + 1, f] = x_after[pl.ds(f, blocks, 8), :]

        t = jnp.where(k < tiles, tiles - 1 - k, k)
        face = jnp.where(k < tiles, t, t - 1)
        over, under = jnp.minimum(t + 1, tiles + 1), jnp.maximum(t - 1, 0)
        for f in range(8):
            w = tile[t, f]
            up = shift_x(tile[over, f], w)
            down = shift_x(w, tile[under, f])
            h = half_slope(w - down, up - w)
            left[t, f] = w + h
            right[t, f] = w - h
        g = face_flux(
            [left[face, f] for f in range(8)],
            [shift_x(right[face + 1, f], right[face, f]) for f in range(8)],
            0,
        )
        for f in range(8):
            faces[face, f] = g[f]

    for copy in y_copies:
        copy.wait()
    lefts, rights, inner_lefts, inner_rights = [], [], [], []
    for f in range(8):
        low_own, high_own = y_send[0, f], y_send[1, f]
        before, after = y_before[f], y_after[f]
        a = jnp.where(even, high_own, turn(before, 72))
        b = jnp.where(even, turn(high_own, -8), turn(before, 64))
        c = jnp.where(even, after, turn(low_own, 72))
        d = jnp.where(even, turn(after, -8), turn(low_own, 64))
        mid = c - b
        h_b, h_c = half_slope(b - a, mid), half_slope(mid, d - c)
        lefts.append(b + h_b)
        rights.append(c - h_c)
        p = inner[f]
        p = jnp.where(even, p, turn(p, -16))
        inner_lefts.append(jnp.where(even, p, c + h_c))
        inner_rights.append(jnp.where(even, b - h_b, p))
    g = face_flux(lefts, rights, 1)
    g_inner = face_flux(inner_lefts, inner_rights, 1)
    for f in range(8):
        between = g[f] - g_inner[f]
        edge[f] = jnp.where(even, between, -between)
        near[f] = jnp.where(even, g_inner[f], -turn(g_inner[f], 16))

    @pl.loop(0, tiles)
    def _(t):
        rim_back = lax.rem(56 + LANES - 16 * t, LANES)
        near_back = lax.rem(48 + LANES - 16 * t, LANES)
        for f in range(8):
            across = faces[t + 1, f]
            across = across - shift_x(across, faces[t, f])
            added = jnp.where(
                y_rim, turn(edge[f], rim_back), jnp.where(y_near, turn(near[f], near_back), 0.0)
            )
            result = across + (change[t, f] + added)
            moved[t, pl.ds(reach * 8 + f, blocks, 8), :] = result

        @pl.when(i > 0)
        def _():
            to_low(t).start()

        @pl.when(i < count_i - 1)
        def _():
            to_high(t).start()

    @pl.loop(0, count_o - 1)
    def _(k):
        out_copy(k).wait()

    row = top_send2[...]
    for k in range(count_o - 1):
        row = jnp.maximum(row, top_in2[k])
    fastest[...] = row

    @pl.when(i > 0)
    def _():
        for t in range(tiles):
            to_low(t).wait_send()
            to_high(t).wait_recv()
        state_low.wait_send()
        state_high.wait_recv()

    @pl.when(i < count_i - 1)
    def _():
        for t in range(tiles):
            to_high(t).wait_send()
            to_low(t).wait_recv()
        state_high.wait_send()
        state_low.wait_recv()


def place_kernel(capacity, moved, state, fastest, run, out, held, out_sem):
    tiles = state.shape[0]
    start = jnp.max(run[pl.ds(0, 1), :])
    count = jnp.max(run[pl.ds(1, 1), :])
    live = lax.broadcasted_iota(jnp.int32, (capacity, LANES), 0) < count
    time_step = COURANT / jnp.max(fastest[...], axis=1, keepdims=True)

    def put(t):
        spot = pl.ds(pl.multiple_of(t * LANES, LANES), LANES)
        return pltpu.make_async_copy(held.at[t], out.at[:, :, spot], out_sem.at[t])

    @pl.loop(0, tiles)
    def _(t):
        rows = [pl.ds(start * 8 + f, capacity, 8) for f in range(8)]
        cons = conserved([state[t, rows[f], :] for f in range(8)])
        for f in range(8):
            held[t, f] = jnp.where(live, cons[f] - time_step * moved[t, rows[f], :], 0.0)
        put(t).start()

    @pl.loop(0, tiles)
    def _(t):
        put(t).wait()


def per_device(count_o, count_i, prim, new_owner, new_slot):
    blocks, cells = prim.shape[1:]
    reach = blocks // 2
    tiles = cells // LANES
    capacity = blocks + 2 * reach
    anywhere = pl.BlockSpec(memory_space=pl.ANY)
    vmem = pl.BlockSpec(memory_space=pltpu.VMEM)
    f32 = jnp.float32
    dma = pltpu.SemaphoreType.DMA

    def room(*lead):
        return pltpu.VMEM(lead + (8, blocks, LANES), f32)

    rows = prim.transpose(1, 0, 2).reshape(blocks * 8, cells)
    handed = pl.pallas_call(
        functools.partial(step_kernel, count_o, count_i, blocks, reach, new_owner.shape[0]),
        out_shape=[
            pltpu.VMEM((tiles, (capacity + 2 * reach) * 8, LANES), f32),
            pltpu.VMEM((tiles, (capacity + 2 * reach) * 8, LANES), f32),
            pltpu.VMEM((1, LANES), f32),
            pltpu.VMEM((2, LANES), jnp.int32),
        ],
        in_specs=[anywhere, anywhere],
        out_specs=[vmem] * 4,
        scratch_shapes=[
            room(tiles + 2),
            room(tiles),
            room(tiles + 2),
            room(tiles + 2),
            room(tiles + 1),
            pltpu.VMEM((blocks * 8, LANES), f32),
            pltpu.VMEM((blocks * 8, LANES), f32),
            room(2),
            room(),
            room(),
            room(),
            room(),
            room(),
            pltpu.VMEM((1, LANES), f32),
            pltpu.VMEM((count_i - 1, 1, LANES), f32),
            pltpu.VMEM((1, LANES), f32),
            pltpu.VMEM((count_o - 1, 1, LANES), f32),
            pltpu.SMEM(new_owner.shape, jnp.int32),
            dma((tiles,)),
            dma,
            dma((2, 2)),
            dma((2, 2)),
            dma((2, count_i - 1)),
            dma((2, count_o - 1)),
            dma((2, tiles)),
            dma((2, tiles)),
            dma((2, 2)),
        ],
        compiler_params=pltpu.CompilerParams(collective_id=0, has_side_effects=True),
        name="step",
    )(rows, new_owner)
    return pl.pallas_call(
        functools.partial(place_kernel, capacity),
        out_shape=jax.ShapeDtypeStruct((8, capacity, cells), f32),
        in_specs=[vmem] * 4,
        out_specs=anywhere,
        scratch_shapes=[pltpu.VMEM((tiles, 8, capacity, LANES), f32), dma((tiles,))],
        name="place",
    )(*[pltpu.with_memory_space_constraint(part, pltpu.VMEM) for part in handed])


def solution(mesh):
    in_specs = (P(None, ("outer", "inner"), None), P(), P())
    out_specs = P(None, ("outer", "inner"), None)
    run = functools.partial(per_device, mesh.shape["outer"], mesh.shape["inner"])
    return jax.shard_map(
        run, mesh=mesh, in_specs=in_specs, out_specs=out_specs, check_vma=False
    )
```
